32 devices in a mesh: dp: 4 (over x, y), sp: 8 (over z, core).
Axes of the slice: x: 2, y: 2, z: 4, core: 2. Of those that a mesh axis runs over, the one named last changes fastest.
Arguments:
- x: bfloat16 [16384, 4096], P(('dp', 'sp')), parts along dimension 0
- gain: bfloat16 [4096], replicated
- wq: bfloat16 [4096, 4096], P('sp')
- wk: bfloat16 [4096, 256], P('sp')
- wv: bfloat16 [4096, 256], P('sp')
- wo: bfloat16 [4096, 4096], P('sp')
Outputs:
- output: bfloat16 [16384, 4096], P(('dp', 'sp')), parts along dimension 0
There are 4 independent parts. The reference program is written for one: setup_inputs(seed, part) draws one part's arguments, and reference() takes and returns one part's arrays. A program takes and returns all parts, laid end to end along the dimension named above; an argument that names none is the same for every part.
All inputs are finite; a program needn't handle non-finite values.
Results may differ from the reference program's by a relative error of at most 0.012.
Values are sent between devices in bfloat16 or wider.
A program may use at most 2 GiB of HBM per device.

```python
import jax
import jax.numpy as jnp
from jax import lax

ROWS = 4096
D = 4096
HEADS = 32
KV_HEADS = 2
HEAD = 128
THETA = 10000


def setup_inputs(seed: int = 0, part: int = 0) -> dict:
    kx, kn, kq, kk, kv, ko = jax.random.split(jax.random.key(seed), 6)

    def weights(key, rows, columns):
        return jax.random.normal(key, (rows, columns), jnp.float32) * rows**-0.5

    drawn = {
        "x": jax.random.normal(jax.random.fold_in(kx, part), (ROWS, D), jnp.float32),
        "gain": 1 + 0.1 * jax.random.normal(kn, (D,), jnp.float32),
        "wq": 2 * weights(kq, D, HEADS * HEAD),
        "wk": 2 * weights(kk, D, KV_HEADS * HEAD),
        "wv": 4 * weights(kv, D, KV_HEADS * HEAD),
        "wo": weights(ko, HEADS * HEAD, D),
    }
    return {k: v.astype(jnp.bfloat16) for k, v in drawn.items()}


def normed(x, gain):
    wide = x.astype(jnp.float32)
    scale = lax.rsqrt(jnp.mean(wide * wide, -1, keepdims=True) + 1e-6)
    return (wide * scale * gain.astype(jnp.float32)).astype(jnp.bfloat16)


def turned(t, place, theta):
    half = t.shape[-1] // 2
    angle = place.astype(jnp.float32)[:, None] * theta ** (-jnp.arange(half, dtype=jnp.float32) / half)
    cos, sin = jnp.cos(angle)[:, None], jnp.sin(angle)[:, None]
    a, b = t[..., :half].astype(jnp.float32), t[..., half:].astype(jnp.float32)
    return jnp.concatenate([a * cos - b * sin, b * cos + a * sin], -1).astype(jnp.bfloat16)


def matmul(a, w):
    return jnp.dot(a, w, preferred_element_type=jnp.float32).astype(jnp.bfloat16)


def einsum(form, a, b):
    return jnp.einsum(form, a.astype(jnp.float32), b.astype(jnp.float32))


def attention(q, k, v):
    scores = einsum("tgsd,ugd->gstu", q, k) * q.shape[-1] ** -0.5
    token = jnp.arange(q.shape[0])
    scores = jnp.where(token[:, None] >= token, scores, -jnp.inf)
    weights = jax.nn.softmax(scores, -1).astype(jnp.bfloat16)
    return einsum("gstu,ugd->tgsd", weights, v).astype(jnp.bfloat16)


def reference(x, gain, wq, wk, wv, wo):
    a, place = normed(x, gain), jnp.arange(ROWS)
    q = turned(matmul(a, wq).reshape(ROWS, HEADS, HEAD), place, THETA).reshape(ROWS, KV_HEADS, -1, HEAD)
    k = turned(matmul(a, wk).reshape(ROWS, KV_HEADS, HEAD), place, THETA)
    v = matmul(a, wv).reshape(ROWS, KV_HEADS, HEAD)
    seen = attention(q, k, v).reshape(ROWS, HEADS * HEAD)
    return (x.astype(jnp.float32) + jnp.dot(seen, wo, preferred_element_type=jnp.float32)).astype(jnp.bfloat16)
```

```python
import functools

import jax
import jax.numpy as jnp
from jax import lax
from jax.experimental import pallas as pl
from jax.experimental.pallas import tpu as pltpu
from jax.sharding import PartitionSpec as P

MESH = pl.DeviceIdType.MESH
HEAD = 128
THETA = 10000
LOG2E = 1.4426950408889634
NEG = -1e30
HIDDEN = 2 * NEG
VMEM = 62 * 2**20

WIDE = 256
OWN = 512
PAIR = 2 * OWN
DIM = 4096
HALF = DIM // 2
NQ = HALF // WIDE
NT = 1 + 2 * NQ
SHARD = DIM // 4
QUARTER = SHARD // 4
EIGHTH = QUARTER // 2
BLOCK = 512
CHUNKS = 4
AHEAD = 3


def _dot(a, b, ca, cb):
    return lax.dot_general(a, b, (((ca,), (cb,)), ((), ())), preferred_element_type=jnp.float32)


def _al(v, n):
    return pl.multiple_of(v, n)


def _kernel(x, gain, cos, sin, wq, wk, wv, wo, out, w, a, q, other, keys, vals, res, top_s, mix_s,
            load_s, swap_s, swap_r, z_s, z_r, rel_s, x_s, y_s, x_r, y_r, xf_s, yf_s, xf_r, yf_r, kv_s, kv_r, kvt_s, kvt_r,
            seen_s, seen_r, xl_s, xw_s, xw_r, rl_s, rw_s, rw_r, out_s, outr_s, outr_r):
    dp, sp = lax.axis_index("dp"), lax.axis_index("sp")
    z, c = sp // 2, sp % 2
    px, py = dp // 2, dp % 2
    xn, yn = (1 - px) * 2 + py, px * 2 + (1 - py)
    diag = (1 - px) * 2 + (1 - py)
    mate = 1 - c

    def at(zz):
        return (dp, zz * 2 + c)

    x_dev, y_dev, mate_dev = (xn, sp), (yn, sp), (dp, z * 2 + mate)

    barrier = pltpu.get_barrier_semaphore()
    for d in (1, 2, 3):
        pl.semaphore_signal(barrier, inc=1, device_id=at((z + d) % 4), device_id_type=MESH)
    for dev in (x_dev, y_dev, mate_dev):
        pl.semaphore_signal(barrier, inc=1, device_id=dev, device_id_type=MESH)
    pl.semaphore_wait(barrier, 6)

    def remote(src, dst, s, r, dev):
        return pltpu.make_async_remote_copy(src_ref=src, dst_ref=dst, send_sem=s, recv_sem=r, device_id=dev, device_id_type=MESH)

    def rows(t, start, n):
        return w.at[t, pl.ds(_al(start, n), n), :]

    def same(t, start, n, s, r, dev):
        return remote(rows(t, start, n), rows(t, start, n), s, r, dev)

    mine = _al(z * SHARD + c * OWN, OWN)

    def parts(t, half):
        if t == 0:
            at_k = pl.ds(_al(half * HEAD, HEAD), HEAD)
            return [(wk.at[:, at_k], pl.ds(0, HEAD)), (wv.at[:, at_k], pl.ds(HEAD, HEAD))]
        src, n = (wq, t - 1) if t <= NQ else (wo, t - 1 - NQ)
        return [(src.at[:, pl.ds(_al(half * HALF + n * WIDE, WIDE), WIDE)], slice(None))]

    def loads(t):
        return [pltpu.make_async_copy(src, w.at[t, pl.ds(mine, OWN), cols], load_s.at[t + i * NT])
                for i, (src, cols) in enumerate(parts(t, c))]

    def swaps(t):
        return [remote(src, w.at[t, pl.ds(mine, OWN), cols], swap_s.at[t + i * NT], swap_r.at[t + i * NT], mate_dev)
                for i, (src, cols) in enumerate(parts(t, mate))]

    own_rows = pl.ds(_al(c * OWN, OWN), OWN)
    x_load = pltpu.make_async_copy(x, a.at[own_rows, :], xl_s)
    x_swap = remote(x, a.at[own_rows, :], xw_s, xw_r, mate_dev)
    r_load = pltpu.make_async_copy(x.at[:, pl.ds(_al(c * HALF, HALF), HALF)], res.at[own_rows, :], rl_s)
    r_swap = remote(x.at[:, pl.ds(_al(mate * HALF, HALF), HALF)], res.at[own_rows, :], rw_s, rw_r, mate_dev)
    for t in range(3):
        for copy in loads(t) + swaps(t):
            copy.start()
    x_load.start()
    x_swap.start()
    for t in range(3, NT):
        for copy in loads(t) + swaps(t):
            copy.start()
    r_load.start()
    r_swap.start()

    def arrived(t):
        pltpu.make_async_copy(wq.at[:, pl.ds(0, WIDE)], w.at[t, pl.ds(mine, OWN), :], load_s.at[t]).wait()
        there = _al(z * SHARD + mate * OWN, OWN)
        remote(w.at[t, pl.ds(there, OWN), :], w.at[t, pl.ds(there, OWN), :], swap_s.at[t], swap_r.at[t], mate_dev).wait()

    my_quarter = dp * QUARTER

    def z_sends(t):
        return [((z != zt) & (z - zt <= 2) & (zt - z <= 2), same(t, z * SHARD + my_quarter, QUARTER, z_s.at[t * 4 + zt], z_r.at[t * 4 + z], at(zt)))
                for zt in range(4)]

    def order(i):
        s1 = 0 if i == 0 else i + 1
        s2 = (3, 1, 0)[i]
        return jnp.where(z == 0, i + 1, jnp.where(z == 1, s1, jnp.where(z == 2, s2, 2 - i)))

    def z_copy(t, i):
        s = order(i)
        return same(t, s * SHARD + my_quarter, QUARTER, z_s.at[t * 4 + z], z_r.at[t * 4 + s], at(z))

    def relay(t):
        far = jnp.where(z == 1, 3, 0)
        return (z == 1) | (z == 2), same(t, far * SHARD + my_quarter, QUARTER, rel_s.at[t], z_r.at[t * 4 + far], at(3 - far))

    def plane(t, i):
        s = order(i)
        row = s * SHARD + my_quarter
        return [same(t, row, QUARTER, x_s.at[t * 3 + i], x_r.at[t * 3 + i], x_dev), same(t, row, QUARTER, y_s.at[t * 3 + i], y_r.at[t * 3 + i], y_dev)]

    def plane_in(t, i):
        row = order(i) * SHARD
        return [same(t, row + xn * QUARTER, QUARTER, x_s.at[t * 3 + i], x_r.at[t * 3 + i], x_dev),
                same(t, row + yn * QUARTER, QUARTER, y_s.at[t * 3 + i], y_r.at[t * 3 + i], y_dev)]

    def onward(t, i):
        row = order(i) * SHARD
        return [same(t, row + xn * QUARTER, EIGHTH, yf_s.at[t * 3 + i], yf_r.at[t * 3 + i], y_dev),
                same(t, row + yn * QUARTER + EIGHTH, EIGHTH, xf_s.at[t * 3 + i], xf_r.at[t * 3 + i], x_dev)]

    def onward_in(t, i):
        row = order(i) * SHARD + diag * QUARTER
        return [same(t, row, EIGHTH, yf_s.at[t * 3 + i], yf_r.at[t * 3 + i], y_dev),
                same(t, row + EIGHTH, EIGHTH, xf_s.at[t * 3 + i], xf_r.at[t * 3 + i], x_dev)]

    step = PAIR // CHUNKS

    def kv_copies(n, zs, zt):
        at_n = pl.ds(_al(zs * PAIR + n * step, step), step)
        k, v, i = keys.at[at_n, :], vals.at[:HEAD, at_n], n * 4
        return [remote(k, k, kv_s.at[i + zt], kv_r.at[i + zs], at(zt)), remote(v, v, kvt_s.at[i + zt], kvt_r.at[i + zs], at(zt))]

    def seen_copy(p):
        here, there = q.at[:, pl.ds(_al(p * WIDE, WIDE), WIDE)], other.at[:, pl.ds(_al(p * WIDE, WIDE), WIDE)]
        return remote(here, there, seen_s.at[p], seen_r.at[p], mate_dev)

    def norm(block):
        at_b = pl.ds(_al(block * 128, 128), 128)
        wide = a[at_b, :].astype(jnp.float32)
        scale = lax.rsqrt(jnp.mean(wide * wide, -1, keepdims=True) + 1e-6)
        a[at_b, :] = (wide * scale * gain[...].astype(jnp.float32)).astype(jnp.bfloat16)

    def turned(t, at_b):
        return (t * cos[at_b, :] + pltpu.roll(t, HEAD // 2, 1) * sin[at_b, :]).astype(jnp.bfloat16)

    def project(t, b):
        at_b = pl.ds(b * BLOCK, BLOCK)
        return at_b, _dot(a[at_b, :], w[t], 1, 0).astype(jnp.bfloat16).astype(jnp.float32)

    def project_kv(b):
        at_b, kv = project(0, b)
        keys[pl.ds(_al(z * PAIR + b * BLOCK, BLOCK), BLOCK), :] = turned(kv[:, :HEAD], at_b)
        vals[:HEAD, pl.ds(_al(z * PAIR + b * BLOCK, BLOCK), BLOCK)] = kv[:, HEAD:].T.astype(jnp.bfloat16)

    def project_q(t, b):
        at_b, got = project(t, b)
        for n in range(2):
            q[at_b, pl.ds(_al((t - 1) * WIDE + n * HEAD, HEAD), HEAD)] = turned(got[:, n * HEAD : (n + 1) * HEAD], at_b)

    e = HEAD**-0.5 * LOG2E

    def attend(p, b):
        at_b = pl.ds(b * BLOCK, BLOCK)
        at_h = [pl.ds(_al(p * WIDE + n * HEAD, HEAD), HEAD) for n in range(2)]
        top_s[...] = jnp.full((2, BLOCK), NEG, jnp.float32)
        mix_s[...] = jnp.zeros((2, HEAD + 8, BLOCK), jnp.float32)

        def block(j, masked):
            here = pl.ds(_al(j * BLOCK, BLOCK), BLOCK)
            scores = [_dot(keys[here, :], q[at_b, at_h[n]], 1, 1) for n in range(2)]
            weights, keeps = [], []
            for n, s in enumerate(scores):
                if masked:
                    ok = lax.broadcasted_iota(jnp.int32, (BLOCK, BLOCK), 1) >= lax.broadcasted_iota(jnp.int32, (BLOCK, BLOCK), 0)
                    s = jnp.where(ok, s, HIDDEN)
                old = top_s[n : n + 1, :]
                top = jnp.maximum(old, s.max(axis=0, keepdims=True))
                top_s[n : n + 1, :] = top
                weights.append(jnp.exp2((s - top) * e).astype(jnp.bfloat16))
                keeps.append(jnp.exp2((old - top) * e))
            for n in range(2):
                values = jnp.concatenate([vals[:, here], jnp.ones((8, BLOCK), jnp.bfloat16)], axis=0)
                mix_s[n] = mix_s[n] * keeps[n] + _dot(values, weights[n], 1, 0)

        lax.fori_loop(0, z * 2 + b, lambda j, _: block(j, False), None)
        block(z * 2 + b, True)
        for n in range(2):
            q[at_b, at_h[n]] = (mix_s[n, :HEAD, :] * (1 / mix_s[n, HEAD : HEAD + 1, :])).T.astype(jnp.bfloat16)

    def finish(t, b):
        core = mate if b == 0 else c
        n = t - 1 - NQ
        at_b, at_n = pl.ds(_al(core * OWN, OWN), OWN), pl.ds(_al(n * WIDE, WIDE), WIDE)
        y = _dot(q[at_b, :], w[t, pl.ds(_al(c * HALF, HALF), HALF), :], 1, 0) + _dot(other[at_b, :], w[t, pl.ds(_al(mate * HALF, HALF), HALF), :], 1, 0)
        res[at_b, at_n] = (res[at_b, at_n].astype(jnp.float32) + y).astype(jnp.bfloat16)

    def out_copy(n, b):
        core = mate if b == 0 else c
        src = res.at[pl.ds(_al(core * OWN, OWN), OWN), pl.ds(_al(n * WIDE, WIDE), WIDE)]
        dst = out.at[:, pl.ds(_al(c * HALF + n * WIDE, WIDE), WIDE)]
        return remote(src, dst, outr_s.at[n], outr_r.at[n], mate_dev) if b == 0 else pltpu.make_async_copy(src, dst, out_s.at[n])

    for t in range(1):
        for copy in loads(t):
            copy.wait()
        for copy in swaps(t):
            copy.wait()
    for t in range(AHEAD):
        if t:
            arrived(t)
        for cond, copy in z_sends(t):
            pl.when(cond)(copy.start)

    def between(v, lo, hi):
        return (v >= lo) & (v <= hi)

    def work(t, slot):
        if slot in (1, 4):
            b = 0 if slot == 1 else 1
            pl.when(t == 2)(lambda: project_kv(b))
            pl.when(between(t, 3, 2 + NQ))(lambda: project_q(t - 2, b))
        if slot in (2, 5):
            b = 0 if slot == 2 else 1

            @pl.when(between(t, 7, 6 + NQ))
            def _():
                attend(t - 7, b)

        if slot == 0:
            @pl.when(t == -1)
            def _():
                x_load.wait()
                x_swap.wait()
                lax.fori_loop(0, PAIR // 128, lambda i, _: norm(i), None)

        n, b = slot // 2, slot % 2
        tile = jnp.where(t <= 16, 9 + (t - 15) * 3 + n, t - 2)

        @pl.when(between(t, 15, 16) | (between(t, 17, 18) & (n == 0)))
        def _():
            finish(tile, b)
            out_copy(tile - 1 - NQ, b).start()

    def tick(t, _):
        for slot in range(6):
            if slot == 0:
                @pl.when(between(t + AHEAD, 3, NT - 1) & (t >= 0))
                def _():
                    arrived(t + AHEAD)
                    for cond, copy in z_sends(t + AHEAD):
                        pl.when(cond)(copy.start)

                @pl.when(between(t, 2, NT + 1))
                def _():
                    for i in range(3):
                        for copy in onward_in(t - 2, i):
                            copy.wait_recv()

                @pl.when(between(t, 3, 2 + CHUNKS))
                def _():
                    for zt in range(1, 4):
                        @pl.when(zt > z)
                        def _():
                            for copy in kv_copies(t - 3, z, zt):
                                copy.start()

                @pl.when(t == 7)
                def _():
                    for n in range(CHUNKS):
                        for zs in range(3):
                            @pl.when(zs < z)
                            def _():
                                for copy in kv_copies(n, zs, z):
                                    copy.wait_recv()

                @pl.when(between(t, 8, 7 + NQ))
                def _():
                    seen_copy(t - 8).start()

                @pl.when(t == 15)
                def _():
                    r_load.wait()
                    r_swap.wait()
                    for p in range(NQ):
                        seen_copy(p).wait_recv()

            if slot < 3:
                @pl.when(between(t + 1, 0, NT - 1))
                def _():
                    z_copy(t + 1, slot).wait_recv()
                    if slot == 2:
                        cond, copy = relay(t + 1)
                        pl.when(cond)(copy.start)
                    for copy in plane(t + 1, slot):
                        copy.start()
            else:
                @pl.when(between(t, 0, NT - 1))
                def _():
                    for copy in plane_in(t, slot - 3):
                        copy.wait_recv()
                    for copy in onward(t, slot - 3):
                        copy.start()
            work(t, slot)
        return _

    lax.fori_loop(-1, NT + 2, tick, None)

    def sent(t, _):
        for cond, copy in z_sends(t):
            pl.when(cond)(copy.wait_send)
        cond, copy = relay(t)
        pl.when(cond)(copy.wait_send)
        for i in range(3):
            for copy in plane(t, i) + onward(t, i):
                copy.wait_send()
        return _

    lax.fori_loop(0, NT, sent, None)
    for n in range(CHUNKS):
        for zt in range(1, 4):
            @pl.when(zt > z)
            def _():
                for copy in kv_copies(n, z, zt):
                    copy.wait_send()
    for p in range(NQ):
        seen_copy(p).wait_send()
        out_copy(p, 0).wait()
        out_copy(p, 1).wait()


def _layer(x, gain, cos, sin, wq, wk, wv, wo):
    dma = lambda n: pltpu.SemaphoreType.DMA((n,))
    one = pltpu.SemaphoreType.DMA
    bf = lambda *s: pltpu.VMEM(s, jnp.bfloat16)
    any_, vmem = pl.BlockSpec(memory_space=pl.ANY), pl.BlockSpec(memory_space=pltpu.VMEM)
    sems = [dma(NT + 1 + NT - 1), dma(2 * NT), dma(2 * NT), dma(4 * NT), dma(4 * NT), dma(NT)] + [dma(3 * NT)] * 8
    sems += [dma(4 * CHUNKS)] * 4 + [dma(NQ)] * 2 + [one] * 6 + [dma(NQ)] * 3
    return pl.pallas_call(
        _kernel,
        out_shape=jax.ShapeDtypeStruct((OWN, DIM), jnp.bfloat16),
        in_specs=[any_, vmem, vmem, vmem, any_, any_, any_, any_],
        out_specs=any_,
        scratch_shapes=[bf(NT, DIM, WIDE), bf(PAIR, DIM), bf(PAIR, HALF), bf(PAIR, HALF), bf(DIM, HEAD), bf(HEAD, DIM), bf(PAIR, HALF),
                        pltpu.VMEM((2, BLOCK), jnp.float32), pltpu.VMEM((2, HEAD + 8, BLOCK), jnp.float32), *sems],
        compiler_params=pltpu.CompilerParams(collective_id=0, has_side_effects=True, vmem_limit_bytes=VMEM),
    )(x, gain, cos, sin, wq, wk, wv, wo)


def solution(mesh):
    def step(x, gain, wq, wk, wv, wo):
        place = (lax.axis_index("sp") // 2) * PAIR + jnp.arange(PAIR)
        half = HEAD // 2
        angle = place.astype(jnp.float32)[:, None] * THETA ** (-jnp.arange(half, dtype=jnp.float32) / half)
        cos, sin = jnp.cos(angle), jnp.sin(angle)
        return _layer(x, gain[None], jnp.concatenate([cos, cos], -1), jnp.concatenate([-sin, sin], -1), wq, wk, wv, wo)

    tokens, whole = P(("dp", "sp"), None), P("sp", None)
    return jax.shard_map(
        step,
        mesh=mesh,
        in_specs=(tokens, P(None), whole, whole, whole, whole),
        out_specs=tokens,
        check_vma=False,
    )
```

```python
import functools

import jax
import jax.numpy as jnp
from jax import lax
from jax.experimental import pallas as pl
from jax.experimental.pallas import tpu as pltpu
from jax.sharding import PartitionSpec as P

MESH = pl.DeviceIdType.MESH
HEAD = 128
THETA = 10000
LOG2E = 1.4426950408889634
NEG = -1e30
HIDDEN = 2 * NEG
VMEM = 62 * 2**20

WIDE = 256
OWN = 512
PAIR = 2 * OWN
DIM = 4096
HALF = DIM // 2
NQ = HALF // WIDE
NT = 1 + 2 * NQ
SHARD = DIM // 4
QUARTER = SHARD // 4
EIGHTH = QUARTER // 2
BLOCK = 512
GROUP = 4
NG = HALF // (GROUP * HEAD)
CHUNKS = 2
AHEAD = 2
START = 6
FREE = NQ + 3
WO = START + 2 * NG


def _dot(a, b, ca, cb):
    return lax.dot_general(a, b, (((ca,), (cb,)), ((), ())), preferred_element_type=jnp.float32)


def _al(v, n):
    return pl.multiple_of(v, n)


def _kernel(x, gain, cos, sin, wq, wk, wv, wo, out, w, a, q, keys, vals, top_s, mix_s, free_s,
            load_s, swap_s, swap_r, z_s, z_r, rel_s, x_s, y_s, x_r, y_r, xf_s, yf_s, xf_r, yf_r, kv_s, kv_r, kvt_s, kvt_r,
            seen_s, seen_r, xl_s, xw_s, xw_r, rl_s, rw_s, rw_r, out_s, outr_s, outr_r):
    dp, sp = lax.axis_index("dp"), lax.axis_index("sp")
    z, c = sp // 2, sp % 2
    px, py = dp // 2, dp % 2
    xn, yn = (1 - px) * 2 + py, px * 2 + (1 - py)
    diag = (1 - px) * 2 + (1 - py)
    mate = 1 - c

    def at(zz):
        return (dp, zz * 2 + c)

    x_dev, y_dev, mate_dev = (xn, sp), (yn, sp), (dp, z * 2 + mate)

    barrier = pltpu.get_barrier_semaphore()
    for d in (1, 2, 3):
        pl.semaphore_signal(barrier, inc=1, device_id=at((z + d) % 4), device_id_type=MESH)
    for dev in (x_dev, y_dev, mate_dev):
        pl.semaphore_signal(barrier, inc=1, device_id=dev, device_id_type=MESH)
    pl.semaphore_wait(barrier, 6)

    def remote(src, dst, s, r, dev):
        return pltpu.make_async_remote_copy(src_ref=src, dst_ref=dst, send_sem=s, recv_sem=r, device_id=dev, device_id_type=MESH)

    def rows(t, start, n):
        return w.at[t, pl.ds(_al(start, n), n), :]

    def same(t, start, n, s, r, dev):
        return remote(rows(t, start, n), rows(t, start, n), s, r, dev)

    mine = _al(z * SHARD + c * OWN, OWN)

    def parts(t, half):
        if t == 0:
            at_k = pl.ds(_al(half * HEAD, HEAD), HEAD)
            return [(wk.at[:, at_k], pl.ds(0, HEAD)), (wv.at[:, at_k], pl.ds(HEAD, HEAD))]
        src, n = (wq, t - 1) if t <= NQ else (wo, t - 1 - NQ)
        return [(src.at[:, pl.ds(_al(half * HALF + n * WIDE, WIDE), WIDE)], slice(None))]

    def loads(t):
        return [pltpu.make_async_copy(src, w.at[t, pl.ds(mine, OWN), cols], load_s.at[t + i * NT])
                for i, (src, cols) in enumerate(parts(t, c))]

    def swaps(t):
        return [remote(src, w.at[t, pl.ds(mine, OWN), cols], swap_s.at[t + i * NT], swap_r.at[t + i * NT], mate_dev)
                for i, (src, cols) in enumerate(parts(t, mate))]

    own_rows = pl.ds(_al(c * OWN, OWN), OWN)
    x_load = pltpu.make_async_copy(x, a.at[own_rows, :], xl_s)
    x_swap = remote(x, a.at[own_rows, :], xw_s, xw_r, mate_dev)
    other, res = a.at[:, pl.ds(0, HALF)], a.at[:, pl.ds(HALF, HALF)]
    r_load = pltpu.make_async_copy(x.at[:, pl.ds(_al(c * HALF, HALF), HALF)], res.at[own_rows, :], rl_s)
    r_swap = remote(x.at[:, pl.ds(_al(mate * HALF, HALF), HALF)], res.at[own_rows, :], rw_s, rw_r, mate_dev)
    for t in range(3):
        for copy in loads(t) + swaps(t):
            copy.start()
    x_load.start()
    x_swap.start()
    for t in range(3, NT):
        for copy in loads(t) + swaps(t):
            copy.start()

    def arrived(t):
        pltpu.make_async_copy(wq.at[:, pl.ds(0, WIDE)], w.at[t, pl.ds(mine, OWN), :], load_s.at[t]).wait()
        there = _al(z * SHARD + mate * OWN, OWN)
        remote(w.at[t, pl.ds(there, OWN), :], w.at[t, pl.ds(there, OWN), :], swap_s.at[t], swap_r.at[t], mate_dev).wait()

    my_quarter = dp * QUARTER

    def z_sends(t):
        return [((z - zt == 1) | (zt - z == 1), same(t, z * SHARD + my_quarter, QUARTER, z_s.at[t * 4 + zt], z_r.at[t * 4 + z], at(zt)))
                for zt in range(4)]

    def order(i):
        s1 = 0 if i == 0 else i + 1
        s2 = (3, 1, 0)[i]
        return jnp.where(z == 0, i + 1, jnp.where(z == 1, s1, jnp.where(z == 2, s2, 2 - i)))

    def z_copy(t, i):
        s = order(i)
        return same(t, s * SHARD + my_quarter, QUARTER, z_s.at[t * 4 + z], z_r.at[t * 4 + s], at(z))

    def relay(t, i):
        src = order(i)
        up = src < z
        on = jnp.where(up, z < 3, z > 0)
        return on, same(t, src * SHARD + my_quarter, QUARTER, rel_s.at[t * 3 + i], z_r.at[t * 4 + src], at(jnp.where(up, z + 1, z - 1)))

    def plane(t, i):
        s = order(i)
        row = s * SHARD + my_quarter
        return [same(t, row, QUARTER, x_s.at[t * 3 + i], x_r.at[t * 3 + i], x_dev), same(t, row, QUARTER, y_s.at[t * 3 + i], y_r.at[t * 3 + i], y_dev)]

    def plane_in(t, i):
        row = order(i) * SHARD
        return [same(t, row + xn * QUARTER, QUARTER, x_s.at[t * 3 + i], x_r.at[t * 3 + i], x_dev),
                same(t, row + yn * QUARTER, QUARTER, y_s.at[t * 3 + i], y_r.at[t * 3 + i], y_dev)]

    def onward(t, i):
        row = order(i) * SHARD
        return [same(t, row + xn * QUARTER, EIGHTH, yf_s.at[t * 3 + i], yf_r.at[t * 3 + i], y_dev),
                same(t, row + yn * QUARTER + EIGHTH, EIGHTH, xf_s.at[t * 3 + i], xf_r.at[t * 3 + i], x_dev)]

    def onward_in(t, i):
        row = order(i) * SHARD + diag * QUARTER
        return [same(t, row, EIGHTH, yf_s.at[t * 3 + i], yf_r.at[t * 3 + i], y_dev),
                same(t, row + EIGHTH, EIGHTH, xf_s.at[t * 3 + i], xf_r.at[t * 3 + i], x_dev)]

    step = PAIR // CHUNKS

    def kv_copies(n, zs):
        at_n = pl.ds(_al(zs * PAIR + n * step, step), step)
        k, v, i = keys.at[at_n, :], vals.at[:HEAD, at_n], n * 4 + zs
        dev = at(jnp.minimum(z + 1, 3))
        return [remote(k, k, kv_s.at[i], kv_r.at[i], dev), remote(v, v, kvt_s.at[i], kvt_r.at[i], dev)]

    def seen_copy(g):
        at_g = pl.ds(_al(g * GROUP * HEAD, GROUP * HEAD), GROUP * HEAD)
        return remote(q.at[:, at_g], other.at[:, at_g], seen_s.at[g], seen_r.at[g], mate_dev)

    def norm(block):
        at_b = pl.ds(_al(block * 128, 128), 128)
        wide = a[at_b, :].astype(jnp.float32)
        scale = lax.rsqrt(jnp.mean(wide * wide, -1, keepdims=True) + 1e-6)
        a[at_b, :] = (wide * scale * gain[...].astype(jnp.float32)).astype(jnp.bfloat16)

    def turned(t, at_b):
        return (t * cos[at_b, :] + pltpu.roll(t, HEAD // 2, 1) * sin[at_b, :]).astype(jnp.bfloat16)

    def project(t, b):
        at_b = pl.ds(b * BLOCK, BLOCK)
        return at_b, _dot(a[at_b, :], w[t], 1, 0).astype(jnp.bfloat16).astype(jnp.float32)

    def project_kv(b):
        at_b, kv = project(0, b)
        keys[pl.ds(_al(z * PAIR + b * BLOCK, BLOCK), BLOCK), :] = turned(kv[:, :HEAD], at_b)
        vals[:HEAD, pl.ds(_al(z * PAIR + b * BLOCK, BLOCK), BLOCK)] = kv[:, HEAD:].T.astype(jnp.bfloat16)

    def project_q(t, b):
        at_b, got = project(t, b)
        for n in range(2):
            q[at_b, pl.ds(_al((t - 1) * WIDE + n * HEAD, HEAD), HEAD)] = turned(got[:, n * HEAD : (n + 1) * HEAD], at_b)

    e = HEAD**-0.5 * LOG2E

    def heads(i):
        g, b = i // 2, i % 2
        return [pl.ds(_al((g * GROUP + n) * HEAD, HEAD), HEAD) for n in range(GROUP)], pl.ds(_al(b * BLOCK, BLOCK), BLOCK)

    def attend(i, first, size, masked):
        at_h, at_b = heads(i)
        here = pl.ds(_al(first, BLOCK), size)
        scores = [_dot(keys[here, :], q[at_b, at_n], 1, 1) for at_n in at_h]
        weights, keeps = [], []
        for n, s in enumerate(scores):
            if masked:
                shape = (size, BLOCK)
                ok = lax.broadcasted_iota(jnp.int32, shape, 1) + (size - BLOCK) >= lax.broadcasted_iota(jnp.int32, shape, 0)
                s = jnp.where(ok, s, HIDDEN)
            old = top_s[n : n + 1, :]
            top = jnp.maximum(old, s.max(axis=0, keepdims=True))
            top_s[n : n + 1, :] = top
            weights.append(jnp.exp2((s - top) * e).astype(jnp.bfloat16))
            keeps.append(jnp.exp2((old - top) * e))
        values = jnp.concatenate([vals[:, here], jnp.ones((8, size), jnp.bfloat16)], axis=0)
        for n in range(GROUP):
            mix_s[n] = mix_s[n] * keeps[n] + _dot(values, weights[n], 1, 0)

    def attend_start():
        top_s[...] = jnp.full((GROUP, BLOCK), NEG, jnp.float32)
        mix_s[...] = jnp.zeros((GROUP, HEAD + 8, BLOCK), jnp.float32)

    def attend_end(i):
        at_h, at_b = heads(i)
        for n in range(GROUP):
            q[at_b, at_h[n]] = (mix_s[n, :HEAD, :] * (1 / mix_s[n, HEAD : HEAD + 1, :])).T.astype(jnp.bfloat16)

    def finish(t, b):
        core = mate if b == 0 else c
        n = t - 1 - NQ
        at_b = pl.ds(_al(core * OWN, OWN), OWN)
        y = _dot(q[at_b, :], w[t, pl.ds(_al(c * HALF, HALF), HALF), :], 1, 0) + _dot(a[at_b, :HALF], w[t, pl.ds(_al(mate * HALF, HALF), HALF), :], 1, 0)
        at_r = pl.ds(_al(HALF + n * WIDE, WIDE), WIDE)
        a[at_b, at_r] = (a[at_b, at_r].astype(jnp.float32) + y).astype(jnp.bfloat16)

    def out_copy(n, b):
        core = mate if b == 0 else c
        src = a.at[pl.ds(_al(core * OWN, OWN), OWN), pl.ds(_al(HALF + n * WIDE, WIDE), WIDE)]
        dst = out.at[:, pl.ds(_al(c * HALF + n * WIDE, WIDE), WIDE)]
        return remote(src, dst, outr_s.at[n], outr_r.at[n], mate_dev) if b == 0 else pltpu.make_async_copy(src, dst, out_s.at[n])

    for t in range(1):
        for copy in loads(t):
            copy.wait()
        for copy in swaps(t):
            copy.wait()
    for t in range(AHEAD):
        if t:
            arrived(t)
        for cond, copy in z_sends(t):
            pl.when(cond)(copy.start)

    def between(v, lo, hi):
        return (v >= lo) & (v <= hi)

    def work(t, slot):
        if slot < 4:
            @pl.when(t == 0)
            def _():
                if slot == 0:
                    x_load.wait()
                    x_swap.wait()
                norm(2 * slot)
                norm(2 * slot + 1)

        if slot == 5:
            @pl.when(t == 1)
            def _():
                for i in range(3):
                    for copy in onward_in(0, i):
                        copy.wait_recv()
                project_kv(0)
                project_kv(1)

        if slot in (1, 4):
            b = slot // 3
            pl.when(between(t, 3, 2 + NQ))(lambda: project_q(t - 2, b))
        step = t - START
        if slot in (0, 2, 3, 5):
            @pl.when(between(step, 0, 2 * NG - 1))
            def _():
                if slot == 0:
                    attend_start()
                if slot < 5:
                    n = (0, 2, 3).index(slot)
                    pl.when(n < z)(lambda: attend(step, 2 * n * BLOCK, 2 * BLOCK, False))
                else:
                    pl.when(step % 2 == 0)(lambda: attend(step, z * PAIR, BLOCK, True))
                    pl.when(step % 2 == 1)(lambda: attend(step, z * PAIR, 2 * BLOCK, True))
                    attend_end(step)

        if slot in (0, 1, 3, 4):
            n, b = slot // 3, slot % 3
            many = between(t, WO, WO + 2)
            tile = jnp.where(many, 1 + NQ + (t - WO) * 2 + n, t - 2)

            @pl.when(many | (between(t, WO + 3, NT + 1) & (n == 0)))
            def _():
                finish(tile, b)
                out_copy(tile - 1 - NQ, b).start()

    def sent(t):
        for cond, copy in z_sends(t):
            pl.when(cond)(copy.wait_send)
        for i in range(3):
            cond, copy = relay(t, i)
            pl.when(cond)(copy.wait_send)
            for copy in plane(t, i) + onward(t, i):
                copy.wait_send()

    def tick(t, _):
        for slot in range(6):
            if slot == 0:
                for far in range(4):
                    zs, n = z - far, t - 2 - far

                    @pl.when((zs >= 0) & between(n, 0, CHUNKS - 1))
                    def _():
                        if far:
                            for copy in kv_copies(n, zs):
                                copy.wait_recv()

                        @pl.when(z < 3)
                        def _():
                            for copy in kv_copies(n, zs):
                                copy.start()

                @pl.when(between(t + AHEAD, AHEAD, NT - 1))
                def _():
                    arrived(t + AHEAD)
                    for cond, copy in z_sends(t + AHEAD):
                        pl.when(cond)(copy.start)

                @pl.when(between(t, 3, NT + 1))
                def _():
                    for i in range(3):
                        for copy in onward_in(t - 2, i):
                            copy.wait_recv()

                @pl.when(t == FREE)
                def _():
                    pl.semaphore_signal(free_s, inc=1, device_id=mate_dev, device_id_type=MESH)

                @pl.when(t == FREE + 1)
                def _():
                    pl.semaphore_wait(free_s, 1)
                    r_load.start()
                    r_swap.start()
                    for g in range(NG - 1):
                        seen_copy(g).start()

                @pl.when(t == WO)
                def _():
                    seen_copy(NG - 1).start()
                    r_load.wait()
                    r_swap.wait()
                    for g in range(NG):
                        seen_copy(g).wait_recv()

            if slot == 5:
                pl.when(between(t, 4, NT + 1))(lambda: sent(t - 4))

            if slot < 3:
                @pl.when(between(t + 1, 0, NT - 1))
                def _():
                    z_copy(t + 1, slot).wait_recv()
                    cond, copy = relay(t + 1, slot)
                    pl.when(cond)(copy.start)
                    for copy in plane(t + 1, slot):
                        copy.start()
            else:
                @pl.when(between(t, 0, NT - 1))
                def _():
                    for copy in plane_in(t, slot - 3):
                        copy.wait_recv()
                    for copy in onward(t, slot - 3):
                        copy.start()
            work(t, slot)
        return _

    lax.fori_loop(-1, NT + 2, tick, None)

    sent(NT - 2)
    sent(NT - 1)
    for n in range(CHUNKS):
        for zs in range(3):
            @pl.when((zs <= z) & (z < 3))
            def _():
                for copy in kv_copies(n, zs):
                    copy.wait_send()
    for g in range(NG):
        seen_copy(g).wait_send()
    for p in range(NQ):
        out_copy(p, 0).wait()
        out_copy(p, 1).wait()


def _layer(x, gain, cos, sin, wq, wk, wv, wo):
    dma = lambda n: pltpu.SemaphoreType.DMA((n,))
    one = pltpu.SemaphoreType.DMA
    bf = lambda *s: pltpu.VMEM(s, jnp.bfloat16)
    any_, vmem = pl.BlockSpec(memory_space=pl.ANY), pl.BlockSpec(memory_space=pltpu.VMEM)
    sems = [dma(NT + 1 + NT - 1), dma(2 * NT), dma(2 * NT), dma(4 * NT), dma(4 * NT), dma(3 * NT)] + [dma(3 * NT)] * 8
    sems += [dma(4 * CHUNKS)] * 4 + [dma(NG)] * 2 + [one] * 6 + [dma(NQ)] * 3
    return pl.pallas_call(
        _kernel,
        out_shape=jax.ShapeDtypeStruct((OWN, DIM), jnp.bfloat16),
        in_specs=[any_, vmem, vmem, vmem, any_, any_, any_, any_],
        out_specs=any_,
        scratch_shapes=[bf(NT, DIM, WIDE), bf(PAIR, DIM), bf(PAIR, HALF), bf(DIM, HEAD), bf(HEAD, DIM),
                        pltpu.VMEM((GROUP, BLOCK), jnp.float32), pltpu.VMEM((GROUP, HEAD + 8, BLOCK), jnp.float32), pltpu.SemaphoreType.REGULAR, *sems],
        compiler_params=pltpu.CompilerParams(collective_id=0, has_side_effects=True, vmem_limit_bytes=VMEM),
    )(x, gain, cos, sin, wq, wk, wv, wo)


def solution(mesh):
    def step(x, gain, wq, wk, wv, wo):
        place = (lax.axis_index("sp") // 2) * PAIR + jnp.arange(PAIR)
        half = HEAD // 2
        angle = place.astype(jnp.float32)[:, None] * THETA ** (-jnp.arange(half, dtype=jnp.float32) / half)
        cos, sin = jnp.cos(angle), jnp.sin(angle)
        return _layer(x, gain[None], jnp.concatenate([cos, cos], -1), jnp.concatenate([-sin, sin], -1), wq, wk, wv, wo)

    tokens, whole = P(("dp", "sp"), None), P("sp", None)
    return jax.shard_map(
        step,
        mesh=mesh,
        in_specs=(tokens, P(None), whole, whole, whole, whole),
        out_specs=tokens,
        check_vma=False,
    )
```

```python
import functools

import jax
import jax.numpy as jnp
from jax import lax
from jax.experimental import pallas as pl
from jax.experimental.pallas import tpu as pltpu
from jax.sharding import PartitionSpec as P

MESH = pl.DeviceIdType.MESH
HEAD = 128
THETA = 10000
LOG2E = 1.4426950408889634
NEG = -1e30
HIDDEN = 2 * NEG
VMEM = 62 * 2**20

WIDE = 256
OWN = 512
PAIR = 2 * OWN
DIM = 4096
HALF = DIM // 2
NQ = HALF // WIDE
NT = 1 + 2 * NQ
SHARD = DIM // 4
QUARTER = SHARD // 4
EIGHTH = QUARTER // 2
BLOCK = 512
GROUP = 4
NG = HALF // (GROUP * HEAD)
CHUNKS = 2
AHEAD = 2
START = 6
LAST = NT - 1
EXTRA = 7
FREE = NQ + 3
WO = START + 2 * NG


def _dot(a, b, ca, cb):
    return lax.dot_general(a, b, (((ca,), (cb,)), ((), ())), preferred_element_type=jnp.float32)


def _al(v, n):
    return pl.multiple_of(v, n)


def _kernel(x, gain, cos, sin, wq, wk, wv, wo, out, w, a, q, keys, vals, top_s, mix_s, free_s,
            load_s, swap_s, swap_r, z_s, z_r, rel_s, x_s, y_s, x_r, y_r, xf_s, yf_s, xf_r, yf_r, kv_s, kv_r, kvt_s, kvt_r, up_s, down_s, more_r,
            seen_s, seen_r, xl_s, xw_s, xw_r, rl_s, rw_s, rw_r, out_s, outr_s, outr_r):
    dp, sp = lax.axis_index("dp"), lax.axis_index("sp")
    z, c = sp // 2, sp % 2
    px, py = dp // 2, dp % 2
    xn, yn = (1 - px) * 2 + py, px * 2 + (1 - py)
    diag = (1 - px) * 2 + (1 - py)
    mate = 1 - c

    def at(zz):
        return (dp, zz * 2 + c)

    x_dev, y_dev, mate_dev = (xn, sp), (yn, sp), (dp, z * 2 + mate)

    barrier = pltpu.get_barrier_semaphore()
    for d in (1, 2, 3):
        pl.semaphore_signal(barrier, inc=1, device_id=at((z + d) % 4), device_id_type=MESH)
    for dev in (x_dev, y_dev, mate_dev):
        pl.semaphore_signal(barrier, inc=1, device_id=dev, device_id_type=MESH)
    pl.semaphore_wait(barrier, 6)

    def remote(src, dst, s, r, dev):
        return pltpu.make_async_remote_copy(src_ref=src, dst_ref=dst, send_sem=s, recv_sem=r, device_id=dev, device_id_type=MESH)

    def rows(t, start, n):
        return w.at[t, pl.ds(_al(start, n), n), :]

    def same(t, start, n, s, r, dev):
        return remote(rows(t, start, n), rows(t, start, n), s, r, dev)

    mine = _al(z * SHARD + c * OWN, OWN)

    def parts(t, half):
        if t == 0:
            at_k = pl.ds(_al(half * HEAD, HEAD), HEAD)
            return [(wk.at[:, at_k], pl.ds(0, HEAD)), (wv.at[:, at_k], pl.ds(HEAD, HEAD))]
        src, n = (wq, t - 1) if t <= NQ else (wo, t - 1 - NQ)
        return [(src.at[:, pl.ds(_al(half * HALF + n * WIDE, WIDE), WIDE)], slice(None))]

    def loads(t):
        return [pltpu.make_async_copy(src, w.at[t, pl.ds(mine, OWN), cols], load_s.at[t + i * NT])
                for i, (src, cols) in enumerate(parts(t, c))]

    def swaps(t):
        return [remote(src, w.at[t, pl.ds(mine, OWN), cols], swap_s.at[t + i * NT], swap_r.at[t + i * NT], mate_dev)
                for i, (src, cols) in enumerate(parts(t, mate))]

    own_rows = pl.ds(_al(c * OWN, OWN), OWN)
    x_load = pltpu.make_async_copy(x, a.at[own_rows, :], xl_s)
    x_swap = remote(x, a.at[own_rows, :], xw_s, xw_r, mate_dev)
    other, res = a.at[:, pl.ds(0, HALF)], a.at[:, pl.ds(HALF, HALF)]
    r_load = pltpu.make_async_copy(x.at[:, pl.ds(_al(c * HALF, HALF), HALF)], res.at[own_rows, :], rl_s)
    r_swap = remote(x.at[:, pl.ds(_al(mate * HALF, HALF), HALF)], res.at[own_rows, :], rw_s, rw_r, mate_dev)
    for t in range(3):
        for copy in loads(t) + swaps(t):
            copy.start()
    x_load.start()
    x_swap.start()
    for t in range(3, NT):
        for copy in loads(t) + swaps(t):
            copy.start()

    def arrived(t):
        pltpu.make_async_copy(wq.at[:, pl.ds(0, WIDE)], w.at[t, pl.ds(mine, OWN), :], load_s.at[t]).wait()
        there = _al(z * SHARD + mate * OWN, OWN)
        remote(w.at[t, pl.ds(there, OWN), :], w.at[t, pl.ds(there, OWN), :], swap_s.at[t], swap_r.at[t], mate_dev).wait()

    my_quarter = dp * QUARTER

    def z_sends(t):
        return [((z - zt == 1) | (zt - z == 1), same(t, z * SHARD + my_quarter, QUARTER, z_s.at[t * 4 + zt], z_r.at[t * 4 + z], at(zt)))
                for zt in range(4)]

    def order(i):
        s1 = 0 if i == 0 else i + 1
        s2 = (3, 1, 0)[i]
        return jnp.where(z == 0, i + 1, jnp.where(z == 1, s1, jnp.where(z == 2, s2, 2 - i)))

    def z_copy(t, i):
        s = order(i)
        return same(t, s * SHARD + my_quarter, QUARTER, z_s.at[t * 4 + z], z_r.at[t * 4 + s], at(z))

    def relay(t, i):
        src = order(i)
        up = src < z
        on = jnp.where(up, z < 3, z > 0)
        return on, same(t, src * SHARD + my_quarter, QUARTER, rel_s.at[t * 3 + i], z_r.at[t * 4 + src], at(jnp.where(up, z + 1, z - 1)))

    def plane(t, i):
        s = order(i)
        row = s * SHARD + my_quarter
        return [same(t, row, QUARTER, x_s.at[t * 3 + i], x_r.at[t * 3 + i], x_dev), same(t, row, QUARTER, y_s.at[t * 3 + i], y_r.at[t * 3 + i], y_dev)]

    def plane_in(t, i):
        row = order(i) * SHARD
        return [same(t, row + xn * QUARTER, QUARTER, x_s.at[t * 3 + i], x_r.at[t * 3 + i], x_dev),
                same(t, row + yn * QUARTER, QUARTER, y_s.at[t * 3 + i], y_r.at[t * 3 + i], y_dev)]

    def onward(t, i):
        row = order(i) * SHARD
        return [same(t, row + xn * QUARTER, EIGHTH, yf_s.at[t * 3 + i], yf_r.at[t * 3 + i], y_dev),
                same(t, row + yn * QUARTER + EIGHTH, EIGHTH, xf_s.at[t * 3 + i], xf_r.at[t * 3 + i], x_dev)]

    def onward_in(t, i):
        row = order(i) * SHARD + diag * QUARTER
        return [same(t, row, EIGHTH, yf_s.at[t * 3 + i], yf_r.at[t * 3 + i], y_dev),
                same(t, row + EIGHTH, EIGHTH, xf_s.at[t * 3 + i], xf_r.at[t * 3 + i], x_dev)]

    step = PAIR // CHUNKS

    def kv_copies(n, zs):
        at_n = pl.ds(_al(zs * PAIR + n * step, step), step)
        k, v, i = keys.at[at_n, :], vals.at[:HEAD, at_n], n * 4 + zs
        dev = at(jnp.minimum(z + 1, 3))
        return [remote(k, k, kv_s.at[i], kv_r.at[i], dev), remote(v, v, kvt_s.at[i], kvt_r.at[i], dev)]

    def more(n, s):
        row, i = s * SHARD + (dp + 1 + n) % 4 * QUARTER, n * 4 + s
        return [((s <= z) & (z < 3), same(LAST, row, QUARTER, up_s.at[i], more_r.at[i], at(jnp.minimum(z + 1, 3)))),
                ((s >= z) & (z > 0), same(LAST, row, QUARTER, down_s.at[i], more_r.at[i], at(jnp.maximum(z - 1, 0))))]

    def seen_copy(g):
        at_g = pl.ds(_al(g * GROUP * HEAD, GROUP * HEAD), GROUP * HEAD)
        return remote(q.at[:, at_g], other.at[:, at_g], seen_s.at[g], seen_r.at[g], mate_dev)

    def norm(block):
        at_b = pl.ds(_al(block * 128, 128), 128)
        wide = a[at_b, :].astype(jnp.float32)
        scale = lax.rsqrt(jnp.mean(wide * wide, -1, keepdims=True) + 1e-6)
        a[at_b, :] = (wide * scale * gain[...].astype(jnp.float32)).astype(jnp.bfloat16)

    def turned(t, at_b):
        return (t * cos[at_b, :] + pltpu.roll(t, HEAD // 2, 1) * sin[at_b, :]).astype(jnp.bfloat16)

    def project(t, b):
        at_b = pl.ds(b * BLOCK, BLOCK)
        return at_b, _dot(a[at_b, :], w[t], 1, 0).astype(jnp.bfloat16).astype(jnp.float32)

    def project_kv(b):
        at_b, kv = project(0, b)
        keys[pl.ds(_al(z * PAIR + b * BLOCK, BLOCK), BLOCK), :] = turned(kv[:, :HEAD], at_b)
        vals[:HEAD, pl.ds(_al(z * PAIR + b * BLOCK, BLOCK), BLOCK)] = kv[:, HEAD:].T.astype(jnp.bfloat16)

    def project_q(t, b):
        at_b, got = project(t, b)
        for n in range(2):
            q[at_b, pl.ds(_al((t - 1) * WIDE + n * HEAD, HEAD), HEAD)] = turned(got[:, n * HEAD : (n + 1) * HEAD], at_b)

    e = HEAD**-0.5 * LOG2E

    def heads(i):
        g, b = i // 2, i % 2
        return [pl.ds(_al((g * GROUP + n) * HEAD, HEAD), HEAD) for n in range(GROUP)], pl.ds(_al(b * BLOCK, BLOCK), BLOCK)

    def attend(i, first, size, masked):
        at_h, at_b = heads(i)
        here = pl.ds(_al(first, BLOCK), size)
        scores = [_dot(keys[here, :], q[at_b, at_n], 1, 1) for at_n in at_h]
        weights, keeps = [], []
        for n, s in enumerate(scores):
            if masked:
                shape = (size, BLOCK)
                ok = lax.broadcasted_iota(jnp.int32, shape, 1) + (size - BLOCK) >= lax.broadcasted_iota(jnp.int32, shape, 0)
                s = jnp.where(ok, s, HIDDEN)
            old = top_s[n : n + 1, :]
            top = jnp.maximum(old, s.max(axis=0, keepdims=True))
            top_s[n : n + 1, :] = top
            weights.append(jnp.exp2((s - top) * e).astype(jnp.bfloat16))
            keeps.append(jnp.exp2((old - top) * e))
        values = jnp.concatenate([vals[:, here], jnp.ones((8, size), jnp.bfloat16)], axis=0)
        for n in range(GROUP):
            mix_s[n] = mix_s[n] * keeps[n] + _dot(values, weights[n], 1, 0)

    def attend_start():
        top_s[...] = jnp.full((GROUP, BLOCK), NEG, jnp.float32)
        mix_s[...] = jnp.zeros((GROUP, HEAD + 8, BLOCK), jnp.float32)

    def attend_end(i):
        at_h, at_b = heads(i)
        for n in range(GROUP):
            q[at_b, at_h[n]] = (mix_s[n, :HEAD, :] * (1 / mix_s[n, HEAD : HEAD + 1, :])).T.astype(jnp.bfloat16)

    def finish(t, b):
        core = mate if b == 0 else c
        n = t - 1 - NQ
        at_b = pl.ds(_al(core * OWN, OWN), OWN)
        y = _dot(q[at_b, :], w[t, pl.ds(_al(c * HALF, HALF), HALF), :], 1, 0) + _dot(a[at_b, :HALF], w[t, pl.ds(_al(mate * HALF, HALF), HALF), :], 1, 0)
        at_r = pl.ds(_al(HALF + n * WIDE, WIDE), WIDE)
        a[at_b, at_r] = (a[at_b, at_r].astype(jnp.float32) + y).astype(jnp.bfloat16)

    def out_copy(n, b):
        core = mate if b == 0 else c
        src = a.at[pl.ds(_al(core * OWN, OWN), OWN), pl.ds(_al(HALF + n * WIDE, WIDE), WIDE)]
        dst = out.at[:, pl.ds(_al(c * HALF + n * WIDE, WIDE), WIDE)]
        return remote(src, dst, outr_s.at[n], outr_r.at[n], mate_dev) if b == 0 else pltpu.make_async_copy(src, dst, out_s.at[n])

    for t in range(1):
        for copy in loads(t):
            copy.wait()
        for copy in swaps(t):
            copy.wait()
    for t in range(AHEAD):
        if t:
            arrived(t)
        for cond, copy in z_sends(t):
            pl.when(cond)(copy.start)

    def between(v, lo, hi):
        return (v >= lo) & (v <= hi)

    def work(t, slot):
        if slot < 4:
            @pl.when(t == 0)
            def _():
                if slot == 0:
                    x_load.wait()
                    x_swap.wait()
                norm(2 * slot)
                norm(2 * slot + 1)

        if slot == 5:
            @pl.when(t == 1)
            def _():
                for i in range(3):
                    for copy in onward_in(0, i):
                        copy.wait_recv()
                project_kv(0)
                project_kv(1)

        if slot in (1, 4):
            b = slot // 3
            pl.when(between(t, 3, 2 + NQ))(lambda: project_q(t - 2, b))
        step = t - START
        if slot in (0, 2, 3, 5):
            @pl.when(between(step, 0, 2 * NG - 1))
            def _():
                if slot == 0:
                    attend_start()
                if slot < 5:
                    n = (0, 2, 3).index(slot)
                    pl.when(n < z)(lambda: attend(step, 2 * n * BLOCK, 2 * BLOCK, False))
                else:
                    pl.when(step % 2 == 0)(lambda: attend(step, z * PAIR, BLOCK, True))
                    pl.when(step % 2 == 1)(lambda: attend(step, z * PAIR, 2 * BLOCK, True))
                    attend_end(step)

        if slot in (0, 1, 3, 4):
            n, b = slot // 3, slot % 3
            many = between(t, WO, WO + 2)
            tile = jnp.where(many, 1 + NQ + (t - WO) * 2 + n, t - 2)

            @pl.when(many | (between(t, WO + 3, NT + 1) & (n == 0)))
            def _():
                finish(tile, b)
                out_copy(tile - 1 - NQ, b).start()

    def sent(t, last=False):
        for cond, copy in z_sends(t):
            pl.when(cond)(copy.wait_send)
        for i in range(3):
            cond, copy = relay(t, i)
            pl.when(cond)(copy.wait_send)
            for copy in [] if last else plane(t, i) + onward(t, i):
                copy.wait_send()

    def tick(t, _):
        for slot in range(6):
            if slot == 0:
                for far in range(4):
                    zs, n = z - far, t - 2 - far

                    @pl.when((zs >= 0) & between(n, 0, CHUNKS - 1))
                    def _():
                        if far:
                            for copy in kv_copies(n, zs):
                                copy.wait_recv()

                        @pl.when(z < 3)
                        def _():
                            for copy in kv_copies(n, zs):
                                copy.start()

                @pl.when(between(t + AHEAD, AHEAD, NT - 1))
                def _():
                    pl.when(t + AHEAD < LAST)(lambda: arrived(t + AHEAD))
                    for cond, copy in z_sends(t + AHEAD):
                        pl.when(cond)(copy.start)

                pl.when(t == EXTRA)(lambda: arrived(LAST))
                for n in range(3):
                    for s in range(4):
                        @pl.when(t - EXTRA - 2 * n == jnp.maximum(z - s, s - z))
                        def _():
                            @pl.when(z != s)
                            def _():
                                more(n, s)[0][1].wait_recv()

                            for cond, copy in more(n, s):
                                pl.when(cond)(copy.start)

                @pl.when(between(t, 3, NT))
                def _():
                    for i in range(3):
                        for copy in onward_in(t - 2, i):
                            copy.wait_recv()

                @pl.when(t == FREE)
                def _():
                    pl.semaphore_signal(free_s, inc=1, device_id=mate_dev, device_id_type=MESH)

                @pl.when(t == FREE + 1)
                def _():
                    pl.semaphore_wait(free_s, 1)
                    r_load.start()
                    r_swap.start()
                    for g in range(NG - 1):
                        seen_copy(g).start()

                @pl.when(t == WO)
                def _():
                    seen_copy(NG - 1).start()
                    r_load.wait()
                    r_swap.wait()
                    for g in range(NG):
                        seen_copy(g).wait_recv()

            if slot == 5:
                pl.when(between(t, 4, NT + 1))(lambda: sent(t - 4))

            if slot < 3:
                @pl.when(between(t + 1, 0, NT - 1))
                def _():
                    z_copy(t + 1, slot).wait_recv()
                    cond, copy = relay(t + 1, slot)
                    pl.when(cond)(copy.start)

                    @pl.when(t + 1 < LAST)
                    def _():
                        for copy in plane(t + 1, slot):
                            copy.start()
            else:
                @pl.when(between(t, 0, LAST - 1))
                def _():
                    for copy in plane_in(t, slot - 3):
                        copy.wait_recv()
                    for copy in onward(t, slot - 3):
                        copy.start()
            work(t, slot)
        return _

    lax.fori_loop(-1, NT + 2, tick, None)

    sent(NT - 2)
    sent(LAST, True)
    for n in range(3):
        for s in range(4):
            for cond, copy in more(n, s):
                pl.when(cond)(copy.wait_send)
    for n in range(CHUNKS):
        for zs in range(3):
            @pl.when((zs <= z) & (z < 3))
            def _():
                for copy in kv_copies(n, zs):
                    copy.wait_send()
    for g in range(NG):
        seen_copy(g).wait_send()
    for p in range(NQ):
        out_copy(p, 0).wait()
        out_copy(p, 1).wait()


def _layer(x, gain, cos, sin, wq, wk, wv, wo):
    dma = lambda n: pltpu.SemaphoreType.DMA((n,))
    one = pltpu.SemaphoreType.DMA
    bf = lambda *s: pltpu.VMEM(s, jnp.bfloat16)
    any_, vmem = pl.BlockSpec(memory_space=pl.ANY), pl.BlockSpec(memory_space=pltpu.VMEM)
    sems = [dma(NT + 1 + NT - 1), dma(2 * NT), dma(2 * NT), dma(4 * NT), dma(4 * NT), dma(3 * NT)] + [dma(3 * NT)] * 8
    sems += [dma(4 * CHUNKS)] * 4 + [dma(12)] * 3 + [dma(NG)] * 2 + [one] * 6 + [dma(NQ)] * 3
    return pl.pallas_call(
        _kernel,
        out_shape=jax.ShapeDtypeStruct((OWN, DIM), jnp.bfloat16),
        in_specs=[any_, vmem, vmem, vmem, any_, any_, any_, any_],
        out_specs=any_,
        scratch_shapes=[bf(NT, DIM, WIDE), bf(PAIR, DIM), bf(PAIR, HALF), bf(DIM, HEAD), bf(HEAD, DIM),
                        pltpu.VMEM((GROUP, BLOCK), jnp.float32), pltpu.VMEM((GROUP, HEAD + 8, BLOCK), jnp.float32), pltpu.SemaphoreType.REGULAR, *sems],
        compiler_params=pltpu.CompilerParams(collective_id=0, has_side_effects=True, vmem_limit_bytes=VMEM),
    )(x, gain, cos, sin, wq, wk, wv, wo)


def solution(mesh):
    def step(x, gain, wq, wk, wv, wo):
        place = (lax.axis_index("sp") // 2) * PAIR + jnp.arange(PAIR)
        half = HEAD // 2
        angle = place.astype(jnp.float32)[:, None] * THETA ** (-jnp.arange(half, dtype=jnp.float32) / half)
        cos, sin = jnp.cos(angle), jnp.sin(angle)
        return _layer(x, gain[None], jnp.concatenate([cos, cos], -1), jnp.concatenate([-sin, sin], -1), wq, wk, wv, wo)

    tokens, whole = P(("dp", "sp"), None), P("sp", None)
    return jax.shard_map(
        step,
        mesh=mesh,
        in_specs=(tokens, P(None), whole, whole, whole, whole),
        out_specs=tokens,
        check_vma=False,
    )
```
